32 devices in a mesh: row: 4 (over z), col: 8 (over y, x, core).
Axes of the slice: x: 2, y: 2, z: 4, core: 2. Of those that a mesh axis runs over, the one named last changes fastest.
Arguments:
- tokens: bfloat16 [1024, 8192], P('row', 'col'), may hold values from -6 to 6
- gate_frozen_weight: bfloat16 [8192, 28672], P('col', 'row'), may hold values from -0.0625 to 0.0625
- gate_left_factor: bfloat16 [8192, 64], P('col'), may hold values from -0.046875 to 0.046875
- gate_right_factor: bfloat16 [64, 28672], P(None, 'row'), may hold values from -0.75 to 0.75
- gate_column_magnitude: float32 [28672], P('row'), may hold values from 0.5 to 1.5
- up_frozen_weight: bfloat16 [8192, 28672], P('col', 'row'), may hold values from -0.0625 to 0.0625
- up_left_factor: bfloat16 [8192, 64], P('col'), may hold values from -0.046875 to 0.046875
- up_right_factor: bfloat16 [64, 28672], P(None, 'row'), may hold values from -0.75 to 0.75
- up_column_magnitude: float32 [28672], P('row'), may hold values from 0.5 to 1.5
- down_frozen_weight: bfloat16 [28672, 8192], P('row', 'col'), may hold values from -0.03125 to 0.03125
- down_left_factor: bfloat16 [28672, 64], P('row'), may hold values from -0.02734375 to 0.02734375
- down_right_factor: bfloat16 [64, 8192], P(None, 'col'), may hold values from -0.75 to 0.75
- down_column_magnitude: float32 [8192], P('col'), may hold values from 0.5 to 1.5
Outputs:
- mixed: bfloat16 [1024, 8192], P('row', 'col')
The draws below stay inside these ranges and needn't reach their ends.
All inputs are finite; a program needn't handle non-finite values.
Results may differ from the reference program's by a relative error of at most 0.028.
Values may be sent and summed in bfloat16 or wider, within the bound.
A program may use at most 192 MiB of HBM per device.

```python
import jax
import jax.numpy as jnp
from jax import lax

MODEL_WIDTH = 8192
HIDDEN_UNITS = 28672
UPDATE_RANK = 64
TOKENS = 1024
N_ROW = 4
N_COL = 8


def block_levels(own_key, shape, cuts, least, largest):
    def one(axis_at, parts):
        draws = jax.random.uniform(jax.random.fold_in(jax.random.fold_in(own_key, 6), axis_at), (parts,), jnp.float32, least / len(cuts), largest / len(cuts))
        return jnp.repeat(jnp.exp(draws), shape[axis_at] // parts).reshape((-1,) + (1,) * (len(shape) - axis_at - 1))

    loudness = one(*cuts[0])
    for cut in cuts[1:]:
        loudness = loudness * one(*cut)
    return loudness


def normal_values(own_key, shape, deviation, bound, cuts=(), kind=jnp.bfloat16):
    result = deviation * jax.random.normal(own_key, shape, jnp.float32)
    if cuts:
        result = result * block_levels(own_key, shape, cuts, -0.22, 0.18)
    return jnp.clip(result, -bound, bound).astype(kind)


def setup_inputs(seed: int = 0) -> dict:
    keys = jax.random.split(jax.random.key(seed), 14)
    tokens = normal_values(keys[0], (TOKENS, MODEL_WIDTH), 1.0, 6.0, ((0, 4), (1, 8)))
    gate_frozen_weight = normal_values(keys[1], (MODEL_WIDTH, HIDDEN_UNITS), MODEL_WIDTH ** -0.5, 0.0625, ((0, 8), (1, 4)))
    gate_left_factor = normal_values(keys[2], (MODEL_WIDTH, UPDATE_RANK), (0.3 * MODEL_WIDTH ** -0.5), 0.046875, ((0, 8),))
    gate_right_factor = normal_values(keys[3], (UPDATE_RANK, HIDDEN_UNITS), UPDATE_RANK ** -0.5, 0.75, ((1, 4),))
    gate_column_magnitude = jnp.clip(1.0 + 0.1 * jax.random.normal(keys[4], (HIDDEN_UNITS,), jnp.float32), 0.5, 1.5)
    up_frozen_weight = normal_values(keys[5], (MODEL_WIDTH, HIDDEN_UNITS), MODEL_WIDTH ** -0.5, 0.0625, ((0, 8), (1, 4)))
    up_left_factor = normal_values(keys[6], (MODEL_WIDTH, UPDATE_RANK), (0.3 * MODEL_WIDTH ** -0.5), 0.046875, ((0, 8),))
    up_right_factor = normal_values(keys[7], (UPDATE_RANK, HIDDEN_UNITS), UPDATE_RANK ** -0.5, 0.75, ((1, 4),))
    up_column_magnitude = jnp.clip(1.0 + 0.1 * jax.random.normal(keys[8], (HIDDEN_UNITS,), jnp.float32), 0.5, 1.5)
    down_frozen_weight = normal_values(keys[9], (HIDDEN_UNITS, MODEL_WIDTH), HIDDEN_UNITS ** -0.5, 0.03125, ((0, 4), (1, 8)))
    down_left_factor = normal_values(keys[10], (HIDDEN_UNITS, UPDATE_RANK), (0.3 * HIDDEN_UNITS ** -0.5), 0.02734375, ((0, 4),))
    down_right_factor = normal_values(keys[11], (UPDATE_RANK, MODEL_WIDTH), UPDATE_RANK ** -0.5, 0.75, ((1, 8),))
    down_column_magnitude = jnp.clip(1.0 + 0.1 * jax.random.normal(keys[12], (MODEL_WIDTH,), jnp.float32), 0.5, 1.5)
    return dict(tokens=tokens, gate_frozen_weight=gate_frozen_weight, gate_left_factor=gate_left_factor, gate_right_factor=gate_right_factor, gate_column_magnitude=gate_column_magnitude, up_frozen_weight=up_frozen_weight, up_left_factor=up_left_factor, up_right_factor=up_right_factor, up_column_magnitude=up_column_magnitude, down_frozen_weight=down_frozen_weight, down_left_factor=down_left_factor, down_right_factor=down_right_factor, down_column_magnitude=down_column_magnitude)


stability_offset = 1e-06

def column_square_totals(weight, low_b, low_a, blocks):
    height, width = weight.shape
    piece = width // blocks
    weight_blocks = weight.reshape(height, blocks, piece).transpose(1, 0, 2)
    factor_blocks = low_a.reshape(low_a.shape[0], blocks, piece).transpose(1, 0, 2)

    def single(pair):
        merged = pair[0].astype(jnp.float32) + jnp.dot(low_b, pair[1], preferred_element_type=jnp.float32)
        return lax.optimization_barrier(jnp.sum(merged * merged, axis=0))
    return lax.map(single, (weight_blocks, factor_blocks)).reshape(width)

def blocked_direct(inputs, weight, blocks):
    piece = inputs.shape[1] // blocks

    def step(index, total):
        start = (index * piece).astype(jnp.int32)
        left = lax.dynamic_slice_in_dim(inputs, start, piece, 1)
        right = lax.dynamic_slice_in_dim(weight, start, piece, 0)
        rounded = jnp.dot(left, right, preferred_element_type=jnp.float32).astype(jnp.bfloat16)
        rounded = lax.optimization_barrier(rounded)
        return total + rounded.astype(jnp.float32)
    start_total = jnp.zeros((inputs.shape[0], weight.shape[1]), jnp.float32)
    return lax.fori_loop(0, blocks, step, start_total)

def adapted_input(inputs, weight, low_b, low_a, scale):
    direct = blocked_direct(inputs, weight, N_COL)
    coords = jnp.dot(inputs, low_b, preferred_element_type=jnp.float32)
    update = jnp.dot(coords, low_a.astype(jnp.float32), precision=lax.Precision.HIGHEST)
    return (direct + update) * scale[None, :]

def adapted_matrix(inputs, weight, low_b, low_a, scale):
    direct = jnp.dot(inputs, weight, preferred_element_type=jnp.float32)
    coords = jnp.dot(inputs, low_b, preferred_element_type=jnp.float32)
    update = jnp.dot(coords, low_a.astype(jnp.float32), precision=lax.Precision.HIGHEST)
    return (direct + update) * scale[None, :]

def reference(tokens, gate_frozen_weight, gate_left_factor, gate_right_factor, gate_column_magnitude, up_frozen_weight, up_left_factor, up_right_factor, up_column_magnitude, down_frozen_weight, down_left_factor, down_right_factor, down_column_magnitude):
    gate_column_scale = gate_column_magnitude / jnp.sqrt(column_square_totals(gate_frozen_weight, gate_left_factor, gate_right_factor, N_ROW) + stability_offset)
    up_column_scale = up_column_magnitude / jnp.sqrt(column_square_totals(up_frozen_weight, up_left_factor, up_right_factor, N_ROW) + stability_offset)
    down_column_scale = down_column_magnitude / jnp.sqrt(column_square_totals(down_frozen_weight, down_left_factor, down_right_factor, N_COL) + stability_offset)
    gate_preactivation = adapted_input(tokens, gate_frozen_weight, gate_left_factor, gate_right_factor, gate_column_scale)
    up_preactivation = adapted_input(tokens, up_frozen_weight, up_left_factor, up_right_factor, up_column_scale)
    hidden_values = (jax.nn.silu(gate_preactivation) * up_preactivation).astype(jnp.bfloat16)
    mixed = adapted_matrix(hidden_values, down_frozen_weight, down_left_factor, down_right_factor, down_column_scale)
    return mixed.astype(jnp.bfloat16)
```

```python
import functools

import jax
import jax.numpy as jnp
from jax import lax
from jax.experimental import pallas as pl
from jax.experimental.pallas import tpu as pltpu
from jax.sharding import PartitionSpec as P

MESH = pl.DeviceIdType.MESH
F32, BF16 = jnp.float32, jnp.bfloat16
stability_offset = 1e-06
LAG = 2


class Plan:
    def __init__(self, n_row, n_col, tokens, gate, down):
        self.n_row, self.n_col = n_row, n_col
        self.own, self.depth = tokens.shape
        self.hidden = gate.shape[1]
        self.out = down.shape[1]
        self.width = next(t for t in (512, 256, 128) if self.hidden % t == 0)
        self.chunks = self.hidden // self.width
        bits = n_col.bit_length() - 1
        self.nst = bits - 1
        two = (self.own // 2 // 2) >> self.nst
        self.chains = [list(range(1, bits))]
        if two % 16 == 0:
            self.chains.append(list(range(bits - 1, 0, -1)))
        self.nch = len(self.chains)
        self.half = self.own // 2
        self.rows = [self.half // self.nch >> p for p in range(self.nst + 1)]
        self.lead = max(1, self.chunks * 2 // 7)
        self.tail = max(1, self.chunks * 3 // 14)
        self.mid = self.chunks - self.lead - self.tail
        self.units = n_row * self.chunks
        self.at_sum = [1 + LAG * (p + 1) for p in range(self.nst)]
        self.at_spread = [self.at_sum[-1] + LAG * (q + 1) for q in range(self.nst)]
        self.at_down = self.at_spread[-1] + 1
        self.hidden_slots = max(
            LAG + self.at_down - self.at_sum[-1],
            2 * LAG + 2,
        )

    def order(self, u):
        lead, mid, chunks = self.lead, self.mid, self.chunks
        a = lead + 2 * mid
        b = lead + mid + chunks
        c = b + (self.n_row - 2) * chunks
        j = (u - lead) // 2
        odd = (u - lead) % 2
        v = u - b
        dist = jnp.where(
            u < lead,
            0,
            jnp.where(
                u < a,
                1 - odd,
                jnp.where(u < b, 1, jnp.where(u < c, 2 + v // chunks, 0)),
            ),
        )
        chunk = jnp.where(
            u < lead,
            u,
            jnp.where(
                u < a,
                j + odd * lead,
                jnp.where(
                    u < b,
                    u - a + mid,
                    jnp.where(u < c, v % chunks, lead + mid + u - c),
                ),
            ),
        )
        new = jnp.where(
            u < lead,
            1,
            jnp.where(
                u < a,
                odd,
                jnp.where((u < b) & (chunk >= lead + mid), 1, 0),
            ),
        )
        return dist, chunk, new

    def starts(self):
        b = self.lead + self.mid + self.chunks
        return [None, self.lead] + [b + i * self.chunks for i in range(self.n_row - 2)]


def kernel(p, *refs):
    (x_hbm, wg_hbm, wu_hbm, wd_hbm, bg_hbm, bu_hbm, ag_hbm, au_hbm, bd_hbm, ad_hbm, mag_ref, magd_ref,
     out_ref,
     x, wg, wu, wd, bg, bu, ag, au, bd, ad,
     sq_mine, sq_got, scale, sqd_mine, sqd_got, acc, z_send, z_got, prod, r0) = refs[:33]
    nst, nch = p.nst, p.nch
    rest = refs[33:]
    c, r = rest[:nst + 1], rest[nst + 1 : 2 * nst + 1]
    (h, load_sem, w_sem, x_send_sem, x_recv_sem, sq_send_sem, sq_recv_sem, sqd_send_sem, sqd_recv_sem,
     z_send_sem, z_recv_sem, s0_send_sem, s0_recv_sem, s_send_sem, s_recv_sem, g_send_sem, g_recv_sem,
     f_send_sem, f_recv_sem) = rest[2 * nst + 1 :]
    n_row, n_col, width, own, half = p.n_row, p.n_col, p.width, p.own, p.half
    row, col = lax.axis_index("row"), lax.axis_index("col")
    bit = [(col // (1 << b)) % 2 for b in range(nst + 1)]
    across = [col + (1 - 2 * bit[b]) * (1 << b) for b in range(nst + 1)]

    def in_row(d):
        return {"row": lax.rem(row + d, n_row)}

    def in_col(d):
        return {"col": lax.rem(col + d, n_col)}

    def remote(src, dst, send, recv, device):
        return pltpu.make_async_remote_copy(
            src_ref=src, dst_ref=dst, send_sem=send, recv_sem=recv, device_id=device, device_id_type=MESH
        )

    def at(start, size, step):
        return pl.ds(pl.multiple_of(start, step), size)

    barrier = pltpu.get_barrier_semaphore()
    for d in range(1, n_row):
        pl.semaphore_signal(barrier, inc=1, device_id=in_row(d), device_id_type=MESH)
    for d in range(1, n_col):
        pl.semaphore_signal(barrier, inc=1, device_id=in_col(d), device_id_type=MESH)

    def columns(hbm, ref, ch, sem):
        return pltpu.make_async_copy(hbm.at[:, at(ch * width, width, 128)], ref.at[ch], sem)

    def gate_loads(ch):
        return [columns(wg_hbm, wg, ch, w_sem.at[ch, 0]), columns(wu_hbm, wu, ch, w_sem.at[ch, 1]),
                columns(ag_hbm, ag, ch, w_sem.at[ch, 3]), columns(au_hbm, au, ch, w_sem.at[ch, 4])]

    def down_loads(ch):
        part = at(ch * width, width, 16)
        return [pltpu.make_async_copy(wd_hbm.at[part], wd.at[ch], w_sem.at[ch, 2]),
                pltpu.make_async_copy(bd_hbm.at[part], bd.at[ch], w_sem.at[ch, 5])]

    singles = [pltpu.make_async_copy(s, t, load_sem.at[i])
               for i, (s, t) in enumerate(((bg_hbm, bg), (bu_hbm, bu), (x_hbm, x.at[0]), (ad_hbm, ad)))]
    for copy in singles[:2] + gate_loads(0) + singles[2:]:
        copy.start()
    if p.chunks > 1:
        for copy in gate_loads(1):
            copy.start()
    for copy in singles:
        copy.wait()
    pl.semaphore_wait(barrier, n_row + n_col - 2)

    def x_copy(d):
        return remote(x.at[0], x.at[d], x_send_sem.at[d - 1], x_recv_sem.at[d - 1], in_row(n_row - d))

    for d in range(1, n_row):
        x_copy(d).start()

    def merge(w, b, a, rows, tile):
        def step(i, total):
            part = at(i * tile, tile, tile)
            merged = w[part, :].astype(F32) + jnp.dot(b[part, :], a, preferred_element_type=F32)
            w[part, :] = merged.astype(BF16)
            square = merged * merged
            return total + jnp.sum(square.reshape(tile // 8, 8, square.shape[1]), axis=0)

        return lax.fori_loop(0, rows // tile, step, jnp.zeros((8, w.shape[1]), F32))

    def squares_copy(ch, d):
        return remote(sq_mine.at[ch], sq_got.at[ch, d - 1], sq_send_sem.at[ch], sq_recv_sem.at[ch], in_col(d))

    def squares_wait(ch, sem):
        pltpu.make_async_copy(sq_got.at[ch], sq_got.at[ch], sem).wait()

    def swap0(slot):
        return remote(prod.at[slot, at((1 - bit[0]) * half, half, 16), :], r0.at[slot],
                      s0_send_sem.at[slot], s0_recv_sem.at[slot], {"col": across[0]})

    def sum_copy(s, w, u):
        mine, theirs = u % 2, u % (2 * LAG)
        full, part = p.rows[s], p.rows[s + 1]
        b = p.chains[w][s]
        return remote(c[s].at[mine, at(w * full + (1 - bit[b]) * part, part, 16), :],
                      r[s].at[theirs, pl.ds(w * part, part), :],
                      s_send_sem.at[s, w, theirs], s_recv_sem.at[s, w, theirs], {"col": across[b]})

    def segment(w, s):
        return bit[0] * half + w * p.rows[0] + sum(
            bit[p.chains[w][i]] * p.rows[i + 1] for i in range(s)
        )

    def spread_copy(q, w, u):
        s = nst - 1 - q
        slot = u % p.hidden_slots
        b = p.chains[w][s]
        part = h.at[slot, at(segment(w, s + 1), p.rows[s + 1], 16), :]
        return remote(part, part, g_send_sem.at[q, w, slot], g_recv_sem.at[q, w, slot], {"col": across[b]})

    def swap_last(u):
        slot = u % p.hidden_slots
        part = h.at[slot, at(bit[0] * half, half, 16), :]
        return remote(part, part, f_send_sem.at[slot], f_recv_sem.at[slot], {"col": across[0]})

    def z_copy(d):
        return remote(z_send.at[d - 1], z_got.at[d - 1], z_send_sem.at[d - 1], z_recv_sem.at[d - 1], in_row(d))

    def squares_down_copy(d):
        return remote(sqd_mine, sqd_got.at[d - 1], sqd_send_sem.at[d - 1], sqd_recv_sem.at[d - 1], in_row(d))

    def kept(s, w, u):
        full, part = p.rows[s], p.rows[s + 1]
        rows = at(w * full + bit[p.chains[w][s]] * part, part, 16)
        return c[s][u % 2, rows, :].astype(F32) + r[s][u % (2 * LAG), pl.ds(w * part, part), :].astype(F32)

    sqd_mine[...] = jnp.zeros_like(sqd_mine)
    acc[...] = jnp.zeros_like(acc)

    def tick(t, carry):
        def stage(lag, body):
            u = t - lag

            @pl.when((u >= 0) & (u < p.units))
            def _():
                body(u)

        def down(u):
            dist, ch, new = p.order(u)
            swap_last(u).wait()

            @pl.when(new == 1)
            def _():
                for copy in down_loads(ch):
                    copy.wait()
                sqd_mine[...] += merge(wd.at[ch], bd.at[ch], ad[...], width, 128)

                @pl.when(ch == p.chunks - 1)
                def _():
                    for d in range(1, n_row):
                        squares_down_copy(d).start()

            which = jnp.where(dist == 0, 0, 1)
            acc[which] += jnp.dot(h[u % p.hidden_slots], wd[ch], preferred_element_type=F32)
            for d in range(1, n_row):
                @pl.when((dist == d) & (ch == p.chunks - 1))
                def _(d=d):
                    z_send[d - 1] = acc[1].astype(BF16)
                    acc[1] = jnp.zeros((own, p.out), F32)
                    z_copy(d).start()

        stage(p.at_down, down)

        def swap_stage(u):
            for w in range(nch):
                spread_copy(nst - 1, w, u).wait()
            swap_last(u).start()

        stage(p.at_spread[-1], swap_stage)

        for q in range(nst - 2, -1, -1):
            def spread_stage(u, q=q):
                for w in range(nch):
                    spread_copy(q, w, u).wait()
                    spread_copy(q + 1, w, u).start()

            stage(p.at_spread[q], spread_stage)

        def act(u):
            _, ch, new = p.order(u)

            @pl.when(new == 1)
            def _():
                squares_wait(ch, sq_send_sem.at[ch])
                squares_wait(ch, sq_recv_sem.at[ch])
                total = sq_mine[ch] + jnp.sum(sq_got[ch], axis=0)
                scale[ch] = mag_ref[ch] / jnp.sqrt(total + stability_offset)

            s = scale[ch]
            for w in range(nch):
                sum_copy(nst - 1, w, u).wait()
                value = kept(nst - 1, w, u)
                gate = value[:, :width] * s[0:1]
                up = value[:, width:] * s[1:2]
                hidden = gate / (1.0 + jnp.exp(-gate)) * up
                h[u % p.hidden_slots, at(segment(w, nst), p.rows[nst], 16), :] = hidden.astype(BF16)
                spread_copy(0, w, u).start()

        stage(p.at_sum[-1], act)

        for s in range(nst - 2, -1, -1):
            def sum_stage(u, s=s):
                for w in range(nch):
                    sum_copy(s, w, u).wait()
                    c[s + 1][u % 2, pl.ds(w * p.rows[s + 1], p.rows[s + 1]), :] = kept(s, w, u).astype(BF16)
                    sum_copy(s + 1, w, u).start()

            stage(p.at_sum[s], sum_stage)

        def first_sum(u):
            slot = u % 2
            swap0(slot).wait()
            rows = p.rows[0]
            for w in range(nch):
                total = prod[slot, at(bit[0] * half + w * rows, rows, 16), :].astype(F32)
                total += r0[slot, pl.ds(w * rows, rows), :].astype(F32)
                c[0][slot, pl.ds(w * rows, rows), :] = total.astype(BF16)
                sum_copy(0, w, u).start()

        stage(1, first_sum)

        def product(u):
            dist, ch, new = p.order(u)
            slot = u % 2
            for d, first in enumerate(p.starts()):
                if d:
                    @pl.when(u == first)
                    def _(d=d):
                        x_copy(d).wait()

            @pl.when(new == 1)
            def _():
                for copy in down_loads(ch):
                    copy.start()

                @pl.when((u > 0) & (ch + 1 < p.chunks))
                def _():
                    for copy in gate_loads(ch + 1):
                        copy.start()

                for copy in gate_loads(ch):
                    copy.wait()
                for i, (w, b, a) in enumerate(((wg, bg, ag), (wu, bu, au))):
                    total = merge(w.at[ch], b, a[ch], p.depth, 128)
                    sq_mine[ch, i : i + 1, :] = jnp.sum(total, axis=0, keepdims=True)
                for d in range(1, n_col):
                    squares_copy(ch, d).start()

            tokens = x[dist]
            prod[slot, :, :width] = jnp.dot(tokens, wg[ch], preferred_element_type=F32).astype(BF16)
            prod[slot, :, width:] = jnp.dot(tokens, wu[ch], preferred_element_type=F32).astype(BF16)
            swap0(slot).start()

        stage(0, product)
        return carry

    lax.fori_loop(0, p.units + p.at_down, tick, 0)

    squares = sqd_mine[...]
    for d in range(1, n_row):
        squares_down_copy(d).wait()
        squares += sqd_got[d - 1]
    down_scale = magd_ref[...] / jnp.sqrt(jnp.sum(squares, axis=0, keepdims=True) + stability_offset)
    for d in range(1, n_row):
        z_copy(d).wait()

    def finish(i, carry):
        part = at(i * 32, 32, 32)
        total = acc[0, part, :]
        for d in range(1, n_row):
            total += z_got[d - 1, part, :].astype(F32)
        out_ref[part, :] = (total * down_scale).astype(BF16)
        return carry

    lax.fori_loop(0, own // 32, finish, 0)


def shards(n_row, n_col, tokens, wg, bg, ag, mg, wu, bu, au, mu, wd, bd, ad, md):
    p = Plan(n_row, n_col, tokens, wg, wd)
    rank = bg.shape[1]
    chunks, width, own, out = p.chunks, p.width, p.own, p.out
    mags = jnp.stack([mg.reshape(chunks, width), mu.reshape(chunks, width)], axis=1)
    dma = pltpu.SemaphoreType.DMA
    nst, nch = p.nst, p.nch
    scratch = [
        pltpu.VMEM((n_row, own, p.depth), BF16),
        pltpu.VMEM((chunks, p.depth, width), BF16),
        pltpu.VMEM((chunks, p.depth, width), BF16),
        pltpu.VMEM((chunks, width, out), BF16),
        pltpu.VMEM((p.depth, rank), BF16),
        pltpu.VMEM((p.depth, rank), BF16),
        pltpu.VMEM((chunks, rank, width), BF16),
        pltpu.VMEM((chunks, rank, width), BF16),
        pltpu.VMEM((chunks, width, rank), BF16),
        pltpu.VMEM((rank, out), BF16),
        pltpu.VMEM((chunks, 2, width), F32),
        pltpu.VMEM((chunks, n_col - 1, 2, width), F32),
        pltpu.VMEM((chunks, 2, width), F32),
        pltpu.VMEM((8, out), F32),
        pltpu.VMEM((n_row - 1, 8, out), F32),
        pltpu.VMEM((2, own, out), F32),
        pltpu.VMEM((n_row - 1, own, out), BF16),
        pltpu.VMEM((n_row - 1, own, out), BF16),
        pltpu.VMEM((2, own, 2 * width), BF16),
        pltpu.VMEM((2, p.half, 2 * width), BF16),
    ]
    scratch += [pltpu.VMEM((2, nch * p.rows[s], 2 * width), BF16) for s in range(nst)]
    scratch += [pltpu.VMEM((2, 16, 128), BF16)]
    scratch += [pltpu.VMEM((2 * LAG, nch * p.rows[s + 1], 2 * width), BF16) for s in range(nst)]
    scratch += [pltpu.VMEM((p.hidden_slots, own, width), BF16)]
    scratch += [
        dma((4,)), dma((chunks, 6)), dma((n_row - 1,)), dma((n_row - 1,)), dma((chunks,)), dma((chunks,)),
        dma((n_row - 1,)), dma((n_row - 1,)), dma((n_row - 1,)), dma((n_row - 1,)), dma((2,)), dma((2,)),
        dma((nst, nch, 2 * LAG)), dma((nst, nch, 2 * LAG)),
        dma((nst, nch, p.hidden_slots)), dma((nst, nch, p.hidden_slots)),
        dma((p.hidden_slots,)), dma((p.hidden_slots,)),
    ]
    anywhere = pl.BlockSpec(memory_space=pl.ANY)
    vmem = pl.BlockSpec(memory_space=pltpu.VMEM)
    return pl.pallas_call(
        functools.partial(kernel, p),
        out_shape=jax.ShapeDtypeStruct((own, out), BF16),
        in_specs=[anywhere] * 10 + [vmem] * 2,
        out_specs=vmem,
        scratch_shapes=scratch,
        compiler_params=pltpu.CompilerParams(
            collective_id=0, has_side_effects=True, vmem_limit_bytes=67043328
        ),
        name="layer",
    )(tokens, wg, wu, wd, bg, bu, ag, au, bd, ad, mags, md.reshape(1, out))


def solution(mesh):
    placed = (
        P("row", "col"),
        P("col", "row"), P("col", None), P(None, "row"), P("row"),
        P("col", "row"), P("col", None), P(None, "row"), P("row"),
        P("row", "col"), P("row", None), P(None, "col"), P("col"),
    )

    def body(*arrays):
        return shards(mesh.shape["row"], mesh.shape["col"], *arrays)

    return jax.shard_map(body, mesh=mesh, in_specs=placed, out_specs=P("row", "col"), check_vma=False)
```
